32 devices in a mesh: dp: 8 (over z, x), expert: 4 (over y, core).
Axes of the slice: x: 2, y: 2, z: 4, core: 2. Of those that a mesh axis runs over, the one named last changes fastest.
Arguments:
- tokens: bfloat16 [4096, 2048], P(('dp', 'expert')), may hold values from -6 to 6
- expert_ids: int32 [4096, 8], P(('dp', 'expert')), may hold values from 0 to 15, all different within a row
- route_probs: float32 [4096, 8], P(('dp', 'expert')), may hold values from 0.05 to 1
- shard_limit: int32 [32, 16], P(('dp', 'expert')), may hold values from 32 to 64
- gate_proj: bfloat16 [32, 2048, 384], P(('dp', 'expert')), may hold values from -0.125 to 0.125
- up_proj: bfloat16 [32, 2048, 384], P(('dp', 'expert')), may hold values from -0.125 to 0.125
- down_proj: bfloat16 [32, 384, 2048], P(('dp', 'expert')), may hold values from -0.21875 to 0.21875
Outputs:
- mixed_out: bfloat16 [4096, 2048], P(('dp', 'expert'))
The draws below stay inside these ranges and needn't reach their ends.
Inputs may be any that keep to these rules, and one draw needn't show every extreme that they name: `expert_ids`: each row names 8 different experts.
All inputs are finite; a program needn't handle non-finite values.
Results may differ from the reference program's by a relative error of at most 0.0095.
Values may be sent and summed in bfloat16 or wider, within the bound.
A program may use at most 64 MiB of HBM per device.

```python
import math
import jax
import jax.numpy as jnp
from jax import lax

D = 2048
FF = 768
TOP = 8
TOK_DEV = 128
EXPERTS = 16
SHARDS = 32
TOKENS = 4096
CAP = 64
COL_CAP = 256
N_DP = 8
N_EXPERT = 4


def draw_shard_limit(key, part):
    key_base = jax.random.fold_in(key, 11)
    key_full = jax.random.fold_in(key, 12)
    drawn_base = jax.random.randint(key_base, (SHARDS, EXPERTS), CAP // 2, CAP + 1)
    full_mark = jax.random.randint(key_full, (SHARDS, EXPERTS), 0, 2)
    return jnp.where(full_mark == 1, CAP, drawn_base).astype(jnp.int32)


def block_levels(key, extent, split, least, largest):
    factor_of = 1.0
    for dim, parts in split:
        heights = jax.random.uniform(jax.random.fold_in(jax.random.fold_in(key, 6), dim), (parts,), jnp.float32, least / len(split), largest / len(split))
        factor_of = factor_of * jnp.repeat(jnp.exp(heights), extent[dim] // parts).reshape((-1,) + (1,) * (len(extent) - 1 - dim))
    return factor_of


def choose_distinct(own_key, rows, number_of, top, lift):
    sequence = jax.random.permutation(jax.random.fold_in(own_key, 1), number_of)
    boost = sequence
    for power in range(3):
        boost = boost * boost // number_of
    boost = boost * lift // number_of
    lots = jax.random.randint(jax.random.fold_in(own_key, 2), (rows, number_of), 0, 4096) + boost
    sure = jax.random.permutation(jax.random.fold_in(own_key, 3), rows)[jnp.arange(number_of) % rows]
    lots = jnp.where(jnp.arange(rows)[:, None] == sure[None, :], 1 << 14, lots)
    merit = lots * number_of + jnp.arange(number_of)
    return lax.top_k(merit.astype(jnp.int32), top)[1].astype(jnp.int32)


def noise(own_key, shape, spread, most, split=(), held_as=jnp.bfloat16):
    factor_of = block_levels(own_key, shape, split, -0.22, 0.18) if split else 1.0
    values = jax.random.normal(own_key, shape, jnp.float32) * spread * factor_of
    return jnp.minimum(jnp.maximum(values, -most), most).astype(held_as)


def setup_inputs(seed: int = 0) -> dict:
    keys = jax.random.split(jax.random.key(seed), 8)
    return {
        "tokens": noise(keys[0], (TOKENS, D), 1.0, 6.0, ((0, 32),)),
        "expert_ids": choose_distinct(keys[1], TOKENS, EXPERTS, TOP, 8192),
        "route_probs": jnp.clip(jnp.exp(math.log(1.0) - 2.9957323 * jax.random.uniform(keys[2], (TOKENS, TOP), jnp.float32) ** block_levels(keys[2], (TOKENS, TOP), ((0, 32),), -0.2, 0.2)), 0.05, 1.0),
        "shard_limit": draw_shard_limit(jax.random.fold_in(keys[7], 71), 0),
        "gate_proj": noise(keys[4], (2 * EXPERTS, D, FF // 2), D ** -0.5, 0.125, ((0, 32),)),
        "up_proj": noise(keys[5], (2 * EXPERTS, D, FF // 2), D ** -0.5, 0.125, ((0, 32),)),
        "down_proj": noise(keys[6], (2 * EXPERTS, FF // 2, D), FF ** -0.5, 0.21875, ((0, 32),)),
    }


def half_pair(rows_in, gate_pair, up_pair, down_pair):
    partials = []
    for half_index in range(2):
        gate_val = jnp.dot(rows_in, gate_pair[half_index], preferred_element_type=jnp.float32)
        up_val = jnp.dot(rows_in, up_pair[half_index], preferred_element_type=jnp.float32)
        hidden = (jax.nn.silu(gate_val) * up_val).astype(jnp.bfloat16)
        partials.append(jnp.dot(hidden, down_pair[half_index], preferred_element_type=jnp.float32).astype(jnp.bfloat16))
    return (partials[0].astype(jnp.float32) + partials[1].astype(jnp.float32)).astype(jnp.bfloat16)


def expert_apply(packed):
    return half_pair(packed[0], packed[1], packed[2], packed[3])


def reference(tokens, expert_ids, route_probs, shard_limit, gate_proj, up_proj, down_proj):
    shards = N_DP * N_EXPERT
    route_ids = expert_ids.reshape(shards, TOK_DEV * TOP)
    onehot = (route_ids[:, :, None] == jnp.arange(EXPERTS, dtype=jnp.int32)[None, None, :]).astype(jnp.int32)
    before = (jnp.cumsum(onehot, axis=1) - onehot).astype(jnp.int32)
    slot_rank = jnp.sum(before * onehot, axis=2).astype(jnp.int32)
    expert_count = jnp.sum(onehot, axis=1).astype(jnp.int32)
    kept_count = jnp.minimum(expert_count, shard_limit)
    count_grid = kept_count.reshape(N_DP, N_EXPERT, EXPERTS)
    offset = (jnp.cumsum(count_grid, axis=0) - count_grid).astype(jnp.int32).reshape(shards, EXPERTS)
    limit_each = jnp.take_along_axis(shard_limit, route_ids, axis=1)
    offset_each = jnp.take_along_axis(offset, route_ids, axis=1)
    slot_global = offset_each + slot_rank
    kept_mask = (slot_rank < limit_each) & (slot_global < COL_CAP)
    column = (jnp.arange(shards, dtype=jnp.int32) % N_EXPERT)[:, None]
    per_expert = N_EXPERT * COL_CAP
    total_slots = EXPERTS * per_expert
    target = jnp.where(kept_mask, route_ids * per_expert + column * COL_CAP + slot_global, total_slots).astype(jnp.int32)
    target = target.reshape(shards * TOK_DEV, TOP)
    kept_rows = kept_mask.reshape(shards * TOK_DEV, TOP)
    buffers = jnp.zeros((total_slots, D), jnp.bfloat16)
    for choice_num in range(TOP):
        buffers = buffers.at[target[:, choice_num]].set(tokens, mode="drop")
    buffers = buffers.reshape(EXPERTS, per_expert, D)
    expert_rows = lax.map(expert_apply, (buffers, gate_proj.reshape(EXPERTS, 2, D, FF // 2), up_proj.reshape(EXPERTS, 2, D, FF // 2), down_proj.reshape(EXPERTS, 2, FF // 2, D)))
    flat_rows = expert_rows.reshape(total_slots, D)
    total = jnp.zeros((shards * TOK_DEV, D), jnp.float32)
    for choice_num in range(TOP):
        index_now = jnp.minimum(target[:, choice_num], total_slots - 1)
        fetched = flat_rows[index_now].astype(jnp.float32)
        weight = route_probs[:, choice_num] * kept_rows[:, choice_num].astype(jnp.float32)
        total = total + weight[:, None] * fetched
    return total.astype(jnp.bfloat16)
```

```python
import jax
import jax.numpy as jnp
from jax import lax
from jax.sharding import PartitionSpec as P

BF = jnp.bfloat16
F32 = jnp.float32
CHUNKS = 2


def swap_cores(block, col_size):
    return lax.ppermute(block, "expert", [(c, c ^ 1) for c in range(col_size)])


def turn(block, col_size, by):
    route = [(c, (c + 2 * by) % col_size) for c in range(col_size)]
    return lax.ppermute(block, "expert", route)


def slot_matrices(ids, probs, limits, col_cap, per_row):
    dp_size, tok_rows, _ = ids.shape
    count_y = per_row
    first = lax.axis_index("dp") * per_row
    here = lax.axis_index("expert") // 2
    wanted = first + lax.rem(here + jnp.arange(count_y, dtype=jnp.int32), count_y)
    match = ids[None] == wanted.astype(F32)[:, None, None, None]
    chosen = jnp.sum(match.astype(F32), axis=3)
    weight = jnp.sum(jnp.where(match, probs[None], 0.0), axis=3)
    lower = (jnp.arange(tok_rows)[:, None] < jnp.arange(tok_rows)[None, :]).astype(BF)
    rank = jnp.dot(
        chosen.reshape(-1, tok_rows).astype(BF), lower, preferred_element_type=F32
    ).reshape(chosen.shape)
    pick = (jnp.arange(limits.shape[1], dtype=jnp.int32)[None, :] == wanted[:, None]).astype(F32)
    limit = jnp.sum(pick[:, None, :] * limits[None], axis=2)
    kept = jnp.minimum(jnp.sum(chosen, axis=2), limit)
    earlier = (jnp.arange(dp_size)[:, None] < jnp.arange(dp_size)[None, :]).astype(F32)
    offset = jnp.sum(kept[:, :, None] * earlier[None], axis=1)
    slot = offset[:, :, None] + rank
    keep = (chosen > 0) & (rank < limit[:, :, None]) & (slot < col_cap)
    slot = jnp.where(keep, slot, float(col_cap)).astype(jnp.int32).reshape(count_y, 1, -1)
    weight = weight.reshape(count_y, 1, -1)
    spot = jnp.arange(col_cap, dtype=jnp.int32)[None, :, None] == slot
    return spot.astype(BF), jnp.where(spot, weight, 0.0).astype(BF)


def on_device(tokens, expert_ids, route_probs, shard_limit, gate_proj, up_proj, down_proj):
    tok_rows, width = tokens.shape
    top = expert_ids.shape[1]
    experts = shard_limit.shape[1]
    dp_size = lax.axis_size("dp")
    col_size = lax.axis_size("expert")
    per_row = col_size // 2
    capacity = tok_rows * top // experts
    col_cap = dp_size * capacity // 2
    part = width // CHUNKS

    used = 2 * top + experts
    meta = jnp.concatenate(
        [
            expert_ids.astype(BF),
            route_probs.astype(BF),
            jnp.broadcast_to(shard_limit.astype(BF), (tok_rows, experts)),
            jnp.zeros((tok_rows, -used % 128), BF),
        ],
        axis=1,
    )
    first = lax.all_gather(
        jnp.concatenate([tokens[:, :part], meta], axis=1), "dp", axis=0, tiled=True
    )
    columns = [first[:, :part]]
    for n in range(1, CHUNKS):
        columns.append(
            lax.all_gather(tokens[:, n * part : (n + 1) * part], "dp", axis=0, tiled=True)
        )
    info = first[:, part:].reshape(dp_size, tok_rows, -1).astype(F32)
    spots, weights = slot_matrices(
        info[:, :, :top],
        info[:, :, top : 2 * top],
        info[:, 0, 2 * top : used],
        col_cap,
        per_row,
    )

    gate_half, up_half, down_half = gate_proj[0], up_proj[0], down_proj[0]
    stacks = []
    for n in range(CHUNKS):
        slots = jnp.einsum("rst,td->rsd", spots, columns[n], preferred_element_type=F32).astype(BF)
        held = [slots[0]] + [turn(slots[r], col_size, r) for r in range(1, per_row)]
        held = jnp.concatenate(held, axis=0)
        stacks.append(jnp.concatenate([held, swap_cores(held, col_size)], axis=0))
    rows = jnp.concatenate(stacks, axis=1)
    gate_val = jnp.dot(rows, gate_half, preferred_element_type=F32)
    up_val = jnp.dot(rows, up_half, preferred_element_type=F32)
    hidden = (jax.nn.silu(gate_val) * up_val).astype(BF)

    own = per_row * col_cap
    outs = []
    for n in range(CHUNKS):
        partial = jnp.dot(
            hidden, down_half[:, n * part : (n + 1) * part], preferred_element_type=F32
        ).astype(BF)
        back = swap_cores(partial[own:], col_size)
        merged = (partial[:own].astype(F32) + back.astype(F32)).astype(BF)
        merged = merged.reshape(per_row, col_cap, part)
        home = [merged[0]] + [turn(merged[r], col_size, -r) for r in range(1, per_row)]
        home = jnp.stack(home, axis=0)
        mixed = jnp.einsum("rst,rsd->td", weights, home, preferred_element_type=F32).astype(BF)
        outs.append(lax.psum_scatter(mixed, "dp", scatter_dimension=0, tiled=True))
    return jnp.concatenate(outs, axis=1)


def solution(mesh):
    rows = P(("dp", "expert"), None)
    blocks = P(("dp", "expert"), None, None)
    return jax.shard_map(
        on_device,
        mesh=mesh,
        in_specs=(rows, rows, rows, rows, blocks, blocks, blocks),
        out_specs=rows,
        check_vma=False,
    )
```

```python
import functools

import jax
import jax.numpy as jnp
from jax import lax
from jax.experimental import pallas as pl
from jax.experimental.pallas import tpu as pltpu
from jax.sharding import PartitionSpec as P

BF = jnp.bfloat16
F32 = jnp.float32
CHUNKS = 2


class Wires:
    def __init__(self, ssem, rsem):
        self.ssem, self.rsem = ssem, rsem
        self.count = 0
        self.sent = []

    def lane(self):
        self.count += 1
        return self.count - 1

    def copy(self, src, dst, lane, to):
        return pltpu.make_async_remote_copy(
            src_ref=src,
            dst_ref=dst,
            send_sem=self.ssem.at[lane],
            recv_sem=self.rsem.at[lane],
            device_id={"dp": to},
            device_id_type=pl.DeviceIdType.MESH,
        )

    def send(self, src, dst, lane, to):
        moved = self.copy(src, dst, lane, to)
        moved.start()
        self.sent.append(moved)

    def arrive(self, dst, lane, to):
        self.copy(dst, dst, lane, to).wait_recv()

    def finish(self):
        for moved in self.sent:
            moved.wait_send()


def places(ring):
    me = lax.axis_index("dp")
    z, x = lax.div(me, 2), lax.rem(me, 2)
    ahead = lax.rem(z + 1, ring) * 2 + x
    behind = lax.rem(z + ring - 1, ring) * 2 + x
    return z, x, ahead, behind, z * 2 + 1 - x


def greet(peers):
    barrier = pltpu.get_barrier_semaphore()
    for peer in peers:
        pl.semaphore_signal(
            barrier, inc=1, device_id={"dp": peer}, device_id_type=pl.DeviceIdType.MESH
        )
    pl.semaphore_wait(barrier, len(peers))


def gather_kernel(ring, src, out, ssem, rsem, own_sem):
    z, x, ahead, behind, other = places(ring)
    greet((ahead, behind, other))
    rows = src.shape[0]
    piece = rows // 4
    wires = Wires(ssem, rsem)
    to = [ahead, behind]

    def at(zz, xx, k):
        start = pl.multiple_of((zz * 2 + xx) * rows + k * piece, piece)
        return out.at[pl.ds(start, piece)]

    def back(k, s):
        return lax.rem(z + (ring - s if k % 2 == 0 else s), ring)

    own = [src.at[pl.ds(k * piece, piece)] for k in range(4)]
    ring_lane = {}
    for k in range(4):
        for s in range(ring - 1):
            ring_lane[k, 0, s] = wires.lane()
            if k >= 2:
                ring_lane[k, 1, s] = wires.lane()
    cross_lane = {}
    for k in range(4):
        for s in range(ring if k < 2 else 1):
            cross_lane[k, s] = wires.lane()

    for k in (2, 3):
        wires.send(own[k], at(z, x, k), cross_lane[k, 0], other)
    for k in range(4):
        wires.send(own[k], at(z, x, k), ring_lane[k, 0, 0], to[k % 2])
    for k in (0, 1):
        wires.send(own[k], at(z, x, k), cross_lane[k, 0], other)
    local = pltpu.make_async_copy(
        src, out.at[pl.ds(pl.multiple_of((z * 2 + x) * rows, rows), rows)], own_sem
    )
    local.start()
    for k in (2, 3):
        block = at(z, 1 - x, k)
        wires.arrive(block, cross_lane[k, 0], other)
        wires.send(block, block, ring_lane[k, 1, 0], to[k % 2])
    for s in range(ring - 1):
        for k in (0, 1):
            block = at(back(k, s + 1), x, k)
            wires.arrive(block, ring_lane[k, 0, s], other)
            if s < ring - 2:
                wires.send(block, block, ring_lane[k, 0, s + 1], to[k % 2])
            wires.send(block, block, cross_lane[k, s + 1], other)
        for j in range(2):
            for k in (2, 3):
                block = at(back(k, s + 1), x if j == 0 else 1 - x, k)
                wires.arrive(block, ring_lane[k, j, s], other)
                if s < ring - 2:
                    wires.send(block, block, ring_lane[k, j, s + 1], to[k % 2])
    for s in range(ring):
        for k in (0, 1):
            wires.arrive(at(back(k, s), 1 - x, k), cross_lane[k, s], other)
    local.wait()
    wires.finish()


def scatter_kernel(ring, part, out, cross_a, ring_a, ring_b, cross_b, ssem, rsem):
    z, x, ahead, behind, other = places(ring)
    greet((ahead, behind, other))
    rows = out.shape[0]
    piece = rows // 4
    wires = Wires(ssem, rsem)
    to = [ahead, behind]

    def at(zz, xx, k):
        start = pl.multiple_of((zz * 2 + xx) * rows + k * piece, piece)
        return part.at[pl.ds(start, piece)]

    def goal(k, s):
        return lax.rem(z + (ring - 1 - s if k % 2 == 0 else 1 + s), ring)

    def total(*refs):
        value = refs[0][...].astype(F32)
        for ref in refs[1:]:
            value = value + ref[...].astype(F32)
        return value.astype(BF)

    lanes = {}
    for k in range(4):
        for s in range(ring - 1):
            lanes[k, 0, s] = wires.lane()
            if k >= 2:
                lanes[k, 1, s] = wires.lane()
        for s in range(ring if k < 2 else 1):
            lanes["c", k, s] = wires.lane()

    for j in range(2):
        for k in (2, 3):
            wires.send(
                at(goal(k, 0), x if j == 0 else 1 - x, k),
                ring_b.at[k - 2, j, 0],
                lanes[k, j, 0],
                to[k % 2],
            )
    for s in range(ring):
        for k in (0, 1):
            wires.send(
                at(goal(k, s), 1 - x, k), cross_a.at[k, s], lanes["c", k, s], other
            )
    for s in range(ring - 1):
        for k in (0, 1):
            mine = cross_a.at[k, s]
            wires.arrive(mine, lanes["c", k, s], other)
            terms = [mine, at(goal(k, s), x, k)]
            if s > 0:
                came = ring_a.at[k, s - 1]
                wires.arrive(came, lanes[k, 0, s - 1], other)
                terms.append(came)
            mine[...] = total(*terms)
            wires.send(mine, ring_a.at[k, s], lanes[k, 0, s], to[k % 2])
        if s > 0:
            for j in (1, 0):
                for k in (2, 3):
                    came = ring_b.at[k - 2, j, s - 1]
                    wires.arrive(came, lanes[k, j, s - 1], other)
                    came[...] = total(came, at(goal(k, s), x if j == 0 else 1 - x, k))
                    wires.send(came, ring_b.at[k - 2, j, s], lanes[k, j, s], to[k % 2])
    for k in (2, 3):
        came = ring_b.at[k - 2, 1, ring - 2]
        wires.arrive(came, lanes[k, 1, ring - 2], other)
        came[...] = total(came, at(z, 1 - x, k))
        wires.send(came, cross_b.at[k - 2], lanes["c", k, 0], other)
    for k in (0, 1):
        wires.arrive(cross_a.at[k, ring - 1], lanes["c", k, ring - 1], other)
        wires.arrive(ring_a.at[k, ring - 2], lanes[k, 0, ring - 2], other)
        out[pl.ds(k * piece, piece)] = total(
            at(z, x, k), cross_a.at[k, ring - 1], ring_a.at[k, ring - 2]
        )
    for k in (2, 3):
        came = ring_b.at[k - 2, 0, ring - 2]
        wires.arrive(came, lanes[k, 0, ring - 2], other)
        wires.arrive(cross_b.at[k - 2], lanes["c", k, 0], other)
        out[pl.ds(k * piece, piece)] = total(at(z, x, k), came, cross_b.at[k - 2])
    wires.finish()


def kernel_params(number):
    return pltpu.CompilerParams(
        collective_id=number, has_side_effects=True, vmem_limit_bytes=48 << 20
    )


VM = pl.BlockSpec(memory_space=pltpu.VMEM)


def gather_dp(block, number):
    dp_size = lax.axis_size("dp")
    ring = dp_size // 2
    count = 8 * ring - 4
    return pl.pallas_call(
        functools.partial(gather_kernel, ring),
        name="gather%d" % number,
        out_shape=jax.ShapeDtypeStruct((dp_size * block.shape[0], block.shape[1]), block.dtype),
        in_specs=[VM],
        out_specs=VM,
        scratch_shapes=[
            pltpu.SemaphoreType.DMA((count,)),
            pltpu.SemaphoreType.DMA((count,)),
            pltpu.SemaphoreType.DMA,
        ],
        compiler_params=kernel_params(number),
        cost_estimate=pl.CostEstimate(flops=0, transcendentals=0, bytes_accessed=60 << 20),
    )(block)


def scatter_dp(parts, number):
    dp_size = lax.axis_size("dp")
    ring = dp_size // 2
    rows, wide = parts.shape[0] // dp_size, parts.shape[1]
    piece = rows // 4
    count = 8 * ring - 4
    return pl.pallas_call(
        functools.partial(scatter_kernel, ring),
        name="scatter%d" % number,
        out_shape=jax.ShapeDtypeStruct((rows, wide), parts.dtype),
        in_specs=[VM],
        out_specs=VM,
        scratch_shapes=[
            pltpu.VMEM((2, ring, piece, wide), BF),
            pltpu.VMEM((2, ring - 1, piece, wide), BF),
            pltpu.VMEM((2, 2, ring - 1, piece, wide), BF),
            pltpu.VMEM((2, piece, wide), BF),
            pltpu.SemaphoreType.DMA((count,)),
            pltpu.SemaphoreType.DMA((count,)),
        ],
        compiler_params=kernel_params(number),
        cost_estimate=pl.CostEstimate(flops=0, transcendentals=0, bytes_accessed=60 << 20),
    )(parts)


def swap_cores(block, col_size):
    return lax.ppermute(block, "expert", [(c, c ^ 1) for c in range(col_size)])


def turn(block, col_size, by):
    route = [(c, (c + 2 * by) % col_size) for c in range(col_size)]
    return lax.ppermute(block, "expert", route)


def slot_matrices(ids, probs, limits, col_cap, per_row):
    dp_size, tok_rows, _ = ids.shape
    count_y = per_row
    first = lax.axis_index("dp") * per_row
    here = lax.axis_index("expert") // 2
    wanted = first + lax.rem(here + jnp.arange(count_y, dtype=jnp.int32), count_y)
    match = ids[None] == wanted.astype(F32)[:, None, None, None]
    chosen = jnp.sum(match.astype(F32), axis=3)
    weight = jnp.sum(jnp.where(match, probs[None], 0.0), axis=3)
    lower = (jnp.arange(tok_rows)[:, None] < jnp.arange(tok_rows)[None, :]).astype(BF)
    rank = jnp.dot(
        chosen.reshape(-1, tok_rows).astype(BF), lower, preferred_element_type=F32
    ).reshape(chosen.shape)
    pick = (jnp.arange(limits.shape[1], dtype=jnp.int32)[None, :] == wanted[:, None]).astype(F32)
    limit = jnp.sum(pick[:, None, :] * limits[None], axis=2)
    kept = jnp.minimum(jnp.sum(chosen, axis=2), limit)
    earlier = (jnp.arange(dp_size)[:, None] < jnp.arange(dp_size)[None, :]).astype(F32)
    offset = jnp.sum(kept[:, :, None] * earlier[None], axis=1)
    slot = offset[:, :, None] + rank
    keep = (chosen > 0) & (rank < limit[:, :, None]) & (slot < col_cap)
    slot = jnp.where(keep, slot, float(col_cap)).astype(jnp.int32).reshape(count_y, 1, -1)
    weight = weight.reshape(count_y, 1, -1)
    spot = jnp.arange(col_cap, dtype=jnp.int32)[None, :, None] == slot
    return spot.astype(BF), jnp.where(spot, weight, 0.0).astype(BF)


def on_device(tokens, expert_ids, route_probs, shard_limit, gate_proj, up_proj, down_proj):
    tok_rows, width = tokens.shape
    top = expert_ids.shape[1]
    experts = shard_limit.shape[1]
    dp_size = lax.axis_size("dp")
    col_size = lax.axis_size("expert")
    per_row = col_size // 2
    capacity = tok_rows * top // experts
    col_cap = dp_size * capacity // 2
    part = width // CHUNKS

    used = 2 * top + experts
    meta = jnp.concatenate(
        [
            expert_ids.astype(BF),
            route_probs.astype(BF),
            jnp.broadcast_to(shard_limit.astype(BF), (tok_rows, experts)),
            jnp.zeros((tok_rows, -used % 128), BF),
        ],
        axis=1,
    )
    first = gather_dp(jnp.concatenate([tokens[:, :part], meta], axis=1), 0)
    columns = [first[:, :part]]
    for n in range(1, CHUNKS):
        columns.append(gather_dp(tokens[:, n * part : (n + 1) * part], 2 * n))
    info = first[:, part:].reshape(dp_size, tok_rows, -1).astype(F32)
    spots, weights = slot_matrices(
        info[:, :, :top],
        info[:, :, top : 2 * top],
        info[:, 0, 2 * top : used],
        col_cap,
        per_row,
    )

    gate_half, up_half, down_half = gate_proj[0], up_proj[0], down_proj[0]
    stacks = []
    for n in range(CHUNKS):
        slots = jnp.einsum("rst,td->rsd", spots, columns[n], preferred_element_type=F32).astype(BF)
        held = [slots[0]] + [turn(slots[r], col_size, r) for r in range(1, per_row)]
        held = jnp.concatenate(held, axis=0)
        stacks.append(jnp.concatenate([held, swap_cores(held, col_size)], axis=0))
    rows = jnp.concatenate(stacks, axis=1)
    gate_val = jnp.dot(rows, gate_half, preferred_element_type=F32)
    up_val = jnp.dot(rows, up_half, preferred_element_type=F32)
    hidden = (jax.nn.silu(gate_val) * up_val).astype(BF)

    own = per_row * col_cap
    outs = []
    for n in range(CHUNKS):
        partial = jnp.dot(
            hidden, down_half[:, n * part : (n + 1) * part], preferred_element_type=F32
        ).astype(BF)
        back = swap_cores(partial[own:], col_size)
        merged = (partial[:own].astype(F32) + back.astype(F32)).astype(BF)
        merged = merged.reshape(per_row, col_cap, part)
        home = [merged[0]] + [turn(merged[r], col_size, -r) for r in range(1, per_row)]
        home = jnp.stack(home, axis=0)
        mixed = jnp.einsum("rst,rsd->td", weights, home, preferred_element_type=F32).astype(BF)
        outs.append(scatter_dp(mixed, 2 * n + 1))
    return jnp.concatenate(outs, axis=1)


def solution(mesh):
    rows = P(("dp", "expert"), None)
    blocks = P(("dp", "expert"), None, None)
    return jax.shard_map(
        on_device,
        mesh=mesh,
        in_specs=(rows, rows, rows, rows, blocks, blocks, blocks),
        out_specs=rows,
        check_vma=False,
    )
```

```python
import functools

import jax
import jax.numpy as jnp
from jax import lax
from jax.experimental import pallas as pl
from jax.experimental.pallas import tpu as pltpu
from jax.sharding import PartitionSpec as P

BF = jnp.bfloat16
F32 = jnp.float32
SIXTEENTHS = (8, 5, 3)


class Wires:
    def __init__(self, ssem, rsem):
        self.ssem, self.rsem = ssem, rsem
        self.count = 0
        self.sent = []

    def lane(self):
        self.count += 1
        return self.count - 1

    def copy(self, src, dst, lane, to):
        return pltpu.make_async_remote_copy(
            src_ref=src,
            dst_ref=dst,
            send_sem=self.ssem.at[lane],
            recv_sem=self.rsem.at[lane],
            device_id={"dp": to},
            device_id_type=pl.DeviceIdType.MESH,
        )

    def send(self, src, dst, lane, to):
        moved = self.copy(src, dst, lane, to)
        moved.start()
        self.sent.append(moved)

    def arrive(self, dst, lane, to):
        self.copy(dst, dst, lane, to).wait_recv()

    def finish(self):
        for moved in self.sent:
            moved.wait_send()


def places(ring):
    me = lax.axis_index("dp")
    z, x = lax.div(me, 2), lax.rem(me, 2)
    ahead = lax.rem(z + 1, ring) * 2 + x
    behind = lax.rem(z + ring - 1, ring) * 2 + x
    return z, x, ahead, behind, z * 2 + 1 - x


def pieces(rows):
    unit = rows // 8
    return [(0, 3 * unit), (3 * unit, 3 * unit), (6 * unit, unit), (7 * unit, unit)]


def greet(peers):
    barrier = pltpu.get_barrier_semaphore()
    for peer in peers:
        pl.semaphore_signal(
            barrier, inc=1, device_id={"dp": peer}, device_id_type=pl.DeviceIdType.MESH
        )
    pl.semaphore_wait(barrier, len(peers))


def gather_kernel(ring, src, out, ssem, rsem, own_sem):
    z, x, ahead, behind, other = places(ring)
    greet((ahead, behind, other))
    rows = src.shape[0]
    spans = pieces(rows)
    wires = Wires(ssem, rsem)
    to = [ahead, behind]

    def at(zz, xx, k):
        begin, count = spans[k]
        start = pl.multiple_of((zz * 2 + xx) * rows + begin, rows // 8)
        return out.at[pl.ds(start, count)]

    def back(k, s):
        return lax.rem(z + (ring - s if k % 2 == 0 else s), ring)

    own = [src.at[pl.ds(*spans[k])] for k in range(4)]
    ring_lane = {}
    for k in range(4):
        for s in range(ring - 1):
            ring_lane[k, 0, s] = wires.lane()
            if k >= 2:
                ring_lane[k, 1, s] = wires.lane()
    cross_lane = {}
    for k in range(4):
        for s in range(ring if k < 2 else 1):
            cross_lane[k, s] = wires.lane()

    for k in (2, 3):
        wires.send(own[k], at(z, x, k), cross_lane[k, 0], other)
    for k in range(4):
        wires.send(own[k], at(z, x, k), ring_lane[k, 0, 0], to[k % 2])
    for k in (0, 1):
        wires.send(own[k], at(z, x, k), cross_lane[k, 0], other)
    local = pltpu.make_async_copy(
        src, out.at[pl.ds(pl.multiple_of((z * 2 + x) * rows, rows), rows)], own_sem
    )
    local.start()
    for k in (2, 3):
        block = at(z, 1 - x, k)
        wires.arrive(block, cross_lane[k, 0], other)
        wires.send(block, block, ring_lane[k, 1, 0], to[k % 2])
    for s in range(ring - 1):
        for k in (0, 1):
            block = at(back(k, s + 1), x, k)
            wires.arrive(block, ring_lane[k, 0, s], other)
            if s < ring - 2:
                wires.send(block, block, ring_lane[k, 0, s + 1], to[k % 2])
            wires.send(block, block, cross_lane[k, s + 1], other)
        for j in range(2):
            for k in (2, 3):
                block = at(back(k, s + 1), x if j == 0 else 1 - x, k)
                wires.arrive(block, ring_lane[k, j, s], other)
                if s < ring - 2:
                    wires.send(block, block, ring_lane[k, j, s + 1], to[k % 2])
    for s in range(ring):
        for k in (0, 1):
            wires.arrive(at(back(k, s), 1 - x, k), cross_lane[k, s], other)
    local.wait()
    wires.finish()


def scatter_kernel(ring, part, out, cross_a, ring_a, ring_b, cross_b, ssem, rsem):
    z, x, ahead, behind, other = places(ring)
    greet((ahead, behind, other))
    rows = out.shape[0]
    spans = pieces(rows)
    wires = Wires(ssem, rsem)
    to = [ahead, behind]

    def at(zz, xx, k):
        begin, count = spans[k]
        start = pl.multiple_of((zz * 2 + xx) * rows + begin, rows // 8)
        return part.at[pl.ds(start, count)]

    def goal(k, s):
        return lax.rem(z + (ring - 1 - s if k % 2 == 0 else 1 + s), ring)

    def total(*refs):
        value = refs[0][...].astype(F32)
        for ref in refs[1:]:
            value = value + ref[...].astype(F32)
        return value.astype(BF)

    lanes = {}
    for k in range(4):
        for s in range(ring - 1):
            lanes[k, 0, s] = wires.lane()
            if k >= 2:
                lanes[k, 1, s] = wires.lane()
        for s in range(ring if k < 2 else 1):
            lanes["c", k, s] = wires.lane()

    for j in range(2):
        for k in (2, 3):
            wires.send(
                at(goal(k, 0), x if j == 0 else 1 - x, k),
                ring_b.at[k - 2, j, 0],
                lanes[k, j, 0],
                to[k % 2],
            )
    for s in range(ring):
        for k in (0, 1):
            wires.send(
                at(goal(k, s), 1 - x, k), cross_a.at[k, s], lanes["c", k, s], other
            )
    for s in range(ring - 1):
        for k in (0, 1):
            mine = cross_a.at[k, s]
            wires.arrive(mine, lanes["c", k, s], other)
            terms = [mine, at(goal(k, s), x, k)]
            if s > 0:
                came = ring_a.at[k, s - 1]
                wires.arrive(came, lanes[k, 0, s - 1], other)
                terms.append(came)
            mine[...] = total(*terms)
            wires.send(mine, ring_a.at[k, s], lanes[k, 0, s], to[k % 2])
        if s > 0:
            for j in (1, 0):
                for k in (2, 3):
                    came = ring_b.at[k - 2, j, s - 1]
                    wires.arrive(came, lanes[k, j, s - 1], other)
                    came[...] = total(came, at(goal(k, s), x if j == 0 else 1 - x, k))
                    wires.send(came, ring_b.at[k - 2, j, s], lanes[k, j, s], to[k % 2])
    for k in (2, 3):
        came = ring_b.at[k - 2, 1, ring - 2]
        wires.arrive(came, lanes[k, 1, ring - 2], other)
        came[...] = total(came, at(z, 1 - x, k))
        wires.send(came, cross_b.at[k - 2], lanes["c", k, 0], other)
    for k in (0, 1):
        wires.arrive(cross_a.at[k, ring - 1], lanes["c", k, ring - 1], other)
        wires.arrive(ring_a.at[k, ring - 2], lanes[k, 0, ring - 2], other)
        out[pl.ds(*spans[k])] = total(
            at(z, x, k), cross_a.at[k, ring - 1], ring_a.at[k, ring - 2]
        )
    for k in (2, 3):
        came = ring_b.at[k - 2, 0, ring - 2]
        wires.arrive(came, lanes[k, 0, ring - 2], other)
        wires.arrive(cross_b.at[k - 2], lanes["c", k, 0], other)
        out[pl.ds(*spans[k])] = total(at(z, x, k), came, cross_b.at[k - 2])
    wires.finish()


def kernel_params(number):
    return pltpu.CompilerParams(
        collective_id=number, has_side_effects=True, vmem_limit_bytes=48 << 20
    )


VM = pl.BlockSpec(memory_space=pltpu.VMEM)


def gather_dp(block, number):
    dp_size = lax.axis_size("dp")
    ring = dp_size // 2
    count = 8 * ring - 4
    return pl.pallas_call(
        functools.partial(gather_kernel, ring),
        name="gather%d" % number,
        out_shape=jax.ShapeDtypeStruct((dp_size * block.shape[0], block.shape[1]), block.dtype),
        in_specs=[VM],
        out_specs=VM,
        scratch_shapes=[
            pltpu.SemaphoreType.DMA((count,)),
            pltpu.SemaphoreType.DMA((count,)),
            pltpu.SemaphoreType.DMA,
        ],
        compiler_params=kernel_params(number),
        cost_estimate=pl.CostEstimate(flops=0, transcendentals=0, bytes_accessed=60 << 20),
    )(block)


def scatter_dp(parts, number):
    dp_size = lax.axis_size("dp")
    ring = dp_size // 2
    rows, wide = parts.shape[0] // dp_size, parts.shape[1]
    (_, long), (_, short) = pieces(rows)[1:3]
    count = 8 * ring - 4
    return pl.pallas_call(
        functools.partial(scatter_kernel, ring),
        name="scatter%d" % number,
        out_shape=jax.ShapeDtypeStruct((rows, wide), parts.dtype),
        in_specs=[VM],
        out_specs=VM,
        scratch_shapes=[
            pltpu.VMEM((2, ring, long, wide), BF),
            pltpu.VMEM((2, ring - 1, long, wide), BF),
            pltpu.VMEM((2, 2, ring - 1, short, wide), BF),
            pltpu.VMEM((2, short, wide), BF),
            pltpu.SemaphoreType.DMA((count,)),
            pltpu.SemaphoreType.DMA((count,)),
        ],
        compiler_params=kernel_params(number),
        cost_estimate=pl.CostEstimate(flops=0, transcendentals=0, bytes_accessed=60 << 20),
    )(parts)


def swap_cores(block, col_size):
    return lax.ppermute(block, "expert", [(c, c ^ 1) for c in range(col_size)])


def turn(block, col_size, by):
    route = [(c, (c + 2 * by) % col_size) for c in range(col_size)]
    return lax.ppermute(block, "expert", route)


def slot_matrices(ids, probs, limits, col_cap, per_row):
    dp_size, tok_rows, _ = ids.shape
    count_y = per_row
    first = lax.axis_index("dp") * per_row
    here = lax.axis_index("expert") // 2
    wanted = first + lax.rem(here + jnp.arange(count_y, dtype=jnp.int32), count_y)
    match = ids[None] == wanted.astype(F32)[:, None, None, None]
    chosen = jnp.sum(match.astype(F32), axis=3)
    weight = jnp.sum(jnp.where(match, probs[None], 0.0), axis=3)
    lower = (jnp.arange(tok_rows)[:, None] < jnp.arange(tok_rows)[None, :]).astype(BF)
    rank = jnp.dot(
        chosen.reshape(-1, tok_rows).astype(BF), lower, preferred_element_type=F32
    ).reshape(chosen.shape)
    pick = (jnp.arange(limits.shape[1], dtype=jnp.int32)[None, :] == wanted[:, None]).astype(F32)
    limit = jnp.sum(pick[:, None, :] * limits[None], axis=2)
    kept = jnp.minimum(jnp.sum(chosen, axis=2), limit)
    earlier = (jnp.arange(dp_size)[:, None] < jnp.arange(dp_size)[None, :]).astype(F32)
    offset = jnp.sum(kept[:, :, None] * earlier[None], axis=1)
    slot = offset[:, :, None] + rank
    keep = (chosen > 0) & (rank < limit[:, :, None]) & (slot < col_cap)
    slot = jnp.where(keep, slot, float(col_cap)).astype(jnp.int32).reshape(count_y, 1, -1)
    weight = weight.reshape(count_y, 1, -1)
    spot = jnp.arange(col_cap, dtype=jnp.int32)[None, :, None] == slot
    return spot.astype(BF), jnp.where(spot, weight, 0.0).astype(BF)


def on_device(tokens, expert_ids, route_probs, shard_limit, gate_proj, up_proj, down_proj):
    tok_rows, width = tokens.shape
    top = expert_ids.shape[1]
    experts = shard_limit.shape[1]
    dp_size = lax.axis_size("dp")
    col_size = lax.axis_size("expert")
    per_row = col_size // 2
    capacity = tok_rows * top // experts
    col_cap = dp_size * capacity // 2
    bounds = [0]
    for share in SIXTEENTHS:
        bounds.append(bounds[-1] + width * share // 16)
    spans = list(zip(bounds[:-1], bounds[1:]))
    part = bounds[1]

    used = 2 * top + experts
    meta = jnp.concatenate(
        [
            expert_ids.astype(BF),
            route_probs.astype(BF),
            jnp.broadcast_to(shard_limit.astype(BF), (tok_rows, experts)),
            jnp.zeros((tok_rows, -used % 128), BF),
        ],
        axis=1,
    )
    first = gather_dp(jnp.concatenate([tokens[:, :part], meta], axis=1), 0)
    columns = [first]
    for n, (low, high) in enumerate(spans[1:], 1):
        block, columns[-1] = lax.optimization_barrier((tokens[:, low:high], columns[-1]))
        columns.append(gather_dp(block, 2 * n))
    first = columns[0]
    columns[0] = first[:, :part]
    info = first[:, part:].reshape(dp_size, tok_rows, -1).astype(F32)
    spots, weights = slot_matrices(
        info[:, :, :top],
        info[:, :, top : 2 * top],
        info[:, 0, 2 * top : used],
        col_cap,
        per_row,
    )

    gate_half, up_half, down_half = gate_proj[0], up_proj[0], down_proj[0]
    stacks = []
    for n in range(len(spans)):
        slots = jnp.einsum("rst,td->rsd", spots, columns[n], preferred_element_type=F32).astype(BF)
        held = [slots[0]] + [turn(slots[r], col_size, r) for r in range(1, per_row)]
        held = jnp.concatenate(held, axis=0)
        stacks.append(jnp.concatenate([held, swap_cores(held, col_size)], axis=0))
    rows = jnp.concatenate(stacks, axis=1)
    gate_val = jnp.dot(rows, gate_half, preferred_element_type=F32)
    up_val = jnp.dot(rows, up_half, preferred_element_type=F32)
    hidden = (jax.nn.silu(gate_val) * up_val).astype(BF)

    own = per_row * col_cap
    homes = []
    for low, high in spans[::-1]:
        partial = jnp.dot(hidden, down_half[:, low:high], preferred_element_type=F32).astype(BF)
        back = swap_cores(partial[own:], col_size)
        merged = (partial[:own].astype(F32) + back.astype(F32)).astype(BF)
        if not homes:
            hidden, merged = lax.optimization_barrier((hidden, merged))
        merged = merged.reshape(per_row, col_cap, high - low)
        home = [merged[0]] + [turn(merged[r], col_size, -r) for r in range(1, per_row)]
        homes.append(jnp.stack(home, axis=0))
    outs = []
    for n, home in enumerate(homes):
        if outs:
            home, outs[-1] = lax.optimization_barrier((home, outs[-1]))
        mixed = jnp.einsum("rst,rsd->td", weights, home, preferred_element_type=F32).astype(BF)
        outs.append(scatter_dp(mixed, 2 * n + 1))
    return jnp.concatenate(outs[::-1], axis=1)


def solution(mesh):
    rows = P(("dp", "expert"), None)
    blocks = P(("dp", "expert"), None, None)
    return jax.shard_map(
        on_device,
        mesh=mesh,
        in_specs=(rows, rows, rows, rows, blocks, blocks, blocks),
        out_specs=rows,
        check_vma=False,
    )
```

```python
import functools

import jax
import jax.numpy as jnp
from jax import lax
from jax.experimental import pallas as pl
from jax.experimental.pallas import tpu as pltpu
from jax.sharding import PartitionSpec as P

BF = jnp.bfloat16
F32 = jnp.float32
SIXTEENTHS = (10, 6)


class Wires:
    def __init__(self, ssem, rsem):
        self.ssem, self.rsem = ssem, rsem
        self.count = 0
        self.sent = []

    def lane(self):
        self.count += 1
        return self.count - 1

    def copy(self, src, dst, lane, to):
        return pltpu.make_async_remote_copy(
            src_ref=src,
            dst_ref=dst,
            send_sem=self.ssem.at[lane],
            recv_sem=self.rsem.at[lane],
            device_id={"dp": to},
            device_id_type=pl.DeviceIdType.MESH,
        )

    def send(self, src, dst, lane, to):
        moved = self.copy(src, dst, lane, to)
        moved.start()
        self.sent.append(moved)

    def arrive(self, dst, lane, to):
        self.copy(dst, dst, lane, to).wait_recv()

    def finish(self):
        for moved in self.sent:
            moved.wait_send()


def places(ring):
    me = lax.axis_index("dp")
    z, x = lax.div(me, 2), lax.rem(me, 2)
    ahead = lax.rem(z + 1, ring) * 2 + x
    behind = lax.rem(z + ring - 1, ring) * 2 + x
    return z, x, ahead, behind, z * 2 + 1 - x


def pieces(rows):
    unit = rows // 8
    return [(0, 3 * unit), (3 * unit, 3 * unit), (6 * unit, unit), (7 * unit, unit)]


def greet(peers):
    barrier = pltpu.get_barrier_semaphore()
    for peer in peers:
        pl.semaphore_signal(
            barrier, inc=1, device_id={"dp": peer}, device_id_type=pl.DeviceIdType.MESH
        )
    pl.semaphore_wait(barrier, len(peers))


def gather_kernel(ring, src, out, ssem, rsem, own_sem):
    z, x, ahead, behind, other = places(ring)
    greet((ahead, behind, other))
    rows = src.shape[0]
    spans = pieces(rows)
    wires = Wires(ssem, rsem)
    to = [ahead, behind]

    def at(zz, xx, k):
        begin, count = spans[k]
        start = pl.multiple_of((zz * 2 + xx) * rows + begin, rows // 8)
        return out.at[pl.ds(start, count)]

    def back(k, s):
        return lax.rem(z + (ring - s if k % 2 == 0 else s), ring)

    own = [src.at[pl.ds(*spans[k])] for k in range(4)]
    ring_lane = {}
    for k in range(4):
        for s in range(ring - 1):
            ring_lane[k, 0, s] = wires.lane()
            if k >= 2:
                ring_lane[k, 1, s] = wires.lane()
    cross_lane = {}
    for k in range(4):
        for s in range(ring if k < 2 else 1):
            cross_lane[k, s] = wires.lane()

    for k in (2, 3):
        wires.send(own[k], at(z, x, k), cross_lane[k, 0], other)
    for k in range(4):
        wires.send(own[k], at(z, x, k), ring_lane[k, 0, 0], to[k % 2])
    for k in (0, 1):
        wires.send(own[k], at(z, x, k), cross_lane[k, 0], other)
    local = pltpu.make_async_copy(
        src, out.at[pl.ds(pl.multiple_of((z * 2 + x) * rows, rows), rows)], own_sem
    )
    local.start()
    for k in (2, 3):
        block = at(z, 1 - x, k)
        wires.arrive(block, cross_lane[k, 0], other)
        wires.send(block, block, ring_lane[k, 1, 0], to[k % 2])
    for s in range(ring - 1):
        for k in (0, 1):
            block = at(back(k, s + 1), x, k)
            wires.arrive(block, ring_lane[k, 0, s], other)
            if s < ring - 2:
                wires.send(block, block, ring_lane[k, 0, s + 1], to[k % 2])
            wires.send(block, block, cross_lane[k, s + 1], other)
        for j in range(2):
            for k in (2, 3):
                block = at(back(k, s + 1), x if j == 0 else 1 - x, k)
                wires.arrive(block, ring_lane[k, j, s], other)
                if s < ring - 2:
                    wires.send(block, block, ring_lane[k, j, s + 1], to[k % 2])
    for s in range(ring):
        for k in (0, 1):
            wires.arrive(at(back(k, s), 1 - x, k), cross_lane[k, s], other)
    local.wait()
    wires.finish()


def scatter_kernel(ring, part, out, cross_a, ring_a, ring_b, cross_b, ssem, rsem):
    z, x, ahead, behind, other = places(ring)
    greet((ahead, behind, other))
    rows = out.shape[0]
    spans = pieces(rows)
    wires = Wires(ssem, rsem)
    to = [ahead, behind]

    def at(zz, xx, k):
        begin, count = spans[k]
        start = pl.multiple_of((zz * 2 + xx) * rows + begin, rows // 8)
        return part.at[pl.ds(start, count)]

    def goal(k, s):
        return lax.rem(z + (ring - 1 - s if k % 2 == 0 else 1 + s), ring)

    def total(*refs):
        value = refs[0][...].astype(F32)
        for ref in refs[1:]:
            value = value + ref[...].astype(F32)
        return value.astype(BF)

    lanes = {}
    for k in range(4):
        for s in range(ring - 1):
            lanes[k, 0, s] = wires.lane()
            if k >= 2:
                lanes[k, 1, s] = wires.lane()
        for s in range(ring if k < 2 else 1):
            lanes["c", k, s] = wires.lane()

    for j in range(2):
        for k in (2, 3):
            wires.send(
                at(goal(k, 0), x if j == 0 else 1 - x, k),
                ring_b.at[k - 2, j, 0],
                lanes[k, j, 0],
                to[k % 2],
            )
    for s in range(ring):
        for k in (0, 1):
            wires.send(
                at(goal(k, s), 1 - x, k), cross_a.at[k, s], lanes["c", k, s], other
            )
    for s in range(ring - 1):
        for k in (0, 1):
            mine = cross_a.at[k, s]
            wires.arrive(mine, lanes["c", k, s], other)
            terms = [mine, at(goal(k, s), x, k)]
            if s > 0:
                came = ring_a.at[k, s - 1]
                wires.arrive(came, lanes[k, 0, s - 1], other)
                terms.append(came)
            mine[...] = total(*terms)
            wires.send(mine, ring_a.at[k, s], lanes[k, 0, s], to[k % 2])
        if s > 0:
            for j in (1, 0):
                for k in (2, 3):
                    came = ring_b.at[k - 2, j, s - 1]
                    wires.arrive(came, lanes[k, j, s - 1], other)
                    came[...] = total(came, at(goal(k, s), x if j == 0 else 1 - x, k))
                    wires.send(came, ring_b.at[k - 2, j, s], lanes[k, j, s], to[k % 2])
    for k in (2, 3):
        came = ring_b.at[k - 2, 1, ring - 2]
        wires.arrive(came, lanes[k, 1, ring - 2], other)
        came[...] = total(came, at(z, 1 - x, k))
        wires.send(came, cross_b.at[k - 2], lanes["c", k, 0], other)
    for k in (0, 1):
        wires.arrive(cross_a.at[k, ring - 1], lanes["c", k, ring - 1], other)
        wires.arrive(ring_a.at[k, ring - 2], lanes[k, 0, ring - 2], other)
        out[pl.ds(*spans[k])] = total(
            at(z, x, k), cross_a.at[k, ring - 1], ring_a.at[k, ring - 2]
        )
    for k in (2, 3):
        came = ring_b.at[k - 2, 0, ring - 2]
        wires.arrive(came, lanes[k, 0, ring - 2], other)
        wires.arrive(cross_b.at[k - 2], lanes["c", k, 0], other)
        out[pl.ds(*spans[k])] = total(at(z, x, k), came, cross_b.at[k - 2])
    wires.finish()


def kernel_params(number):
    return pltpu.CompilerParams(
        collective_id=number, has_side_effects=True, vmem_limit_bytes=48 << 20
    )


VM = pl.BlockSpec(memory_space=pltpu.VMEM)


def gather_dp(block, number):
    dp_size = lax.axis_size("dp")
    ring = dp_size // 2
    count = 8 * ring - 4
    return pl.pallas_call(
        functools.partial(gather_kernel, ring),
        name="gather%d" % number,
        out_shape=jax.ShapeDtypeStruct((dp_size * block.shape[0], block.shape[1]), block.dtype),
        in_specs=[VM],
        out_specs=VM,
        scratch_shapes=[
            pltpu.SemaphoreType.DMA((count,)),
            pltpu.SemaphoreType.DMA((count,)),
            pltpu.SemaphoreType.DMA,
        ],
        compiler_params=kernel_params(number),
        cost_estimate=pl.CostEstimate(flops=0, transcendentals=0, bytes_accessed=60 << 20),
    )(block)


def scatter_dp(parts, number):
    dp_size = lax.axis_size("dp")
    ring = dp_size // 2
    rows, wide = parts.shape[0] // dp_size, parts.shape[1]
    (_, long), (_, short) = pieces(rows)[1:3]
    count = 8 * ring - 4
    return pl.pallas_call(
        functools.partial(scatter_kernel, ring),
        name="scatter%d" % number,
        out_shape=jax.ShapeDtypeStruct((rows, wide), parts.dtype),
        in_specs=[VM],
        out_specs=VM,
        scratch_shapes=[
            pltpu.VMEM((2, ring, long, wide), BF),
            pltpu.VMEM((2, ring - 1, long, wide), BF),
            pltpu.VMEM((2, 2, ring - 1, short, wide), BF),
            pltpu.VMEM((2, short, wide), BF),
            pltpu.SemaphoreType.DMA((count,)),
            pltpu.SemaphoreType.DMA((count,)),
        ],
        compiler_params=kernel_params(number),
        cost_estimate=pl.CostEstimate(flops=0, transcendentals=0, bytes_accessed=60 << 20),
    )(parts)


def swap_cores(block, col_size):
    return lax.ppermute(block, "expert", [(c, c ^ 1) for c in range(col_size)])


def turn(block, col_size, by):
    route = [(c, (c + 2 * by) % col_size) for c in range(col_size)]
    return lax.ppermute(block, "expert", route)


def slot_matrices(ids, probs, limits, col_cap, per_row):
    dp_size, tok_rows, _ = ids.shape
    count_y = per_row
    first = lax.axis_index("dp") * per_row
    here = lax.axis_index("expert") // 2
    wanted = first + lax.rem(here + jnp.arange(count_y, dtype=jnp.int32), count_y)
    match = ids[None] == wanted.astype(F32)[:, None, None, None]
    chosen = jnp.sum(match.astype(F32), axis=3)
    weight = jnp.sum(jnp.where(match, probs[None], 0.0), axis=3)
    lower = (jnp.arange(tok_rows)[:, None] < jnp.arange(tok_rows)[None, :]).astype(BF)
    rank = jnp.dot(
        chosen.reshape(-1, tok_rows).astype(BF), lower, preferred_element_type=F32
    ).reshape(chosen.shape)
    pick = (jnp.arange(limits.shape[1], dtype=jnp.int32)[None, :] == wanted[:, None]).astype(F32)
    limit = jnp.sum(pick[:, None, :] * limits[None], axis=2)
    kept = jnp.minimum(jnp.sum(chosen, axis=2), limit)
    earlier = (jnp.arange(dp_size)[:, None] < jnp.arange(dp_size)[None, :]).astype(F32)
    offset = jnp.sum(kept[:, :, None] * earlier[None], axis=1)
    slot = offset[:, :, None] + rank
    keep = (chosen > 0) & (rank < limit[:, :, None]) & (slot < col_cap)
    slot = jnp.where(keep, slot, float(col_cap)).astype(jnp.int32).reshape(count_y, 1, -1)
    weight = weight.reshape(count_y, 1, -1)
    spot = jnp.arange(col_cap, dtype=jnp.int32)[None, :, None] == slot
    return spot.astype(BF), jnp.where(spot, weight, 0.0).astype(BF)


def on_device(tokens, expert_ids, route_probs, shard_limit, gate_proj, up_proj, down_proj):
    tok_rows, width = tokens.shape
    top = expert_ids.shape[1]
    experts = shard_limit.shape[1]
    dp_size = lax.axis_size("dp")
    col_size = lax.axis_size("expert")
    per_row = col_size // 2
    capacity = tok_rows * top // experts
    col_cap = dp_size * capacity // 2
    bounds = [0]
    for share in SIXTEENTHS:
        bounds.append(bounds[-1] + width * share // 16)
    spans = list(zip(bounds[:-1], bounds[1:]))
    part = bounds[1]

    used = 2 * top + experts
    meta = jnp.concatenate(
        [
            expert_ids.astype(BF),
            route_probs.astype(BF),
            jnp.broadcast_to(shard_limit.astype(BF), (tok_rows, experts)),
            jnp.zeros((tok_rows, -used % 128), BF),
        ],
        axis=1,
    )
    first = gather_dp(jnp.concatenate([tokens[:, :part], meta], axis=1), 0)
    columns = [first]
    for n, (low, high) in enumerate(spans[1:], 1):
        block, columns[-1] = lax.optimization_barrier((tokens[:, low:high], columns[-1]))
        columns.append(gather_dp(block, 2 * n))
    first = columns[0]
    columns[0] = first[:, :part]
    info = first[:, part:].reshape(dp_size, tok_rows, -1).astype(F32)
    spots, weights = slot_matrices(
        info[:, :, :top],
        info[:, :, top : 2 * top],
        info[:, 0, 2 * top : used],
        col_cap,
        per_row,
    )

    gate_half, up_half, down_half = gate_proj[0], up_proj[0], down_proj[0]
    stacks = []
    for n in range(len(spans)):
        slots = jnp.einsum("rst,td->rsd", spots, columns[n], preferred_element_type=F32).astype(BF)
        held = [slots[0]] + [turn(slots[r], col_size, r) for r in range(1, per_row)]
        held = jnp.concatenate(held, axis=0)
        stacks.append(jnp.concatenate([held, swap_cores(held, col_size)], axis=0))
    rows = jnp.concatenate(stacks, axis=1)
    gate_val = jnp.dot(rows, gate_half, preferred_element_type=F32)
    up_val = jnp.dot(rows, up_half, preferred_element_type=F32)
    hidden = (jax.nn.silu(gate_val) * up_val).astype(BF)

    own = per_row * col_cap
    homes = []
    for low, high in spans[::-1]:
        partial = jnp.dot(hidden, down_half[:, low:high], preferred_element_type=F32).astype(BF)
        back = swap_cores(partial[own:], col_size)
        merged = (partial[:own].astype(F32) + back.astype(F32)).astype(BF)
        if not homes:
            hidden, merged = lax.optimization_barrier((hidden, merged))
        merged = merged.reshape(per_row, col_cap, high - low)
        home = [merged[0]] + [turn(merged[r], col_size, -r) for r in range(1, per_row)]
        homes.append(jnp.stack(home, axis=0))
    outs = []
    for n, home in enumerate(homes):
        if outs:
            home, outs[-1] = lax.optimization_barrier((home, outs[-1]))
        mixed = jnp.einsum("rst,rsd->td", weights, home, preferred_element_type=F32).astype(BF)
        outs.append(scatter_dp(mixed, 2 * n + 1))
    return jnp.concatenate(outs[::-1], axis=1)


def solution(mesh):
    rows = P(("dp", "expert"), None)
    blocks = P(("dp", "expert"), None, None)
    return jax.shard_map(
        on_device,
        mesh=mesh,
        in_specs=(rows, rows, rows, rows, blocks, blocks, blocks),
        out_specs=rows,
        check_vma=False,
    )
```
